32 devices in a mesh: tmpl: 8 (over y, x, core), grid: 4 (over z).
Axes of the slice: x: 2, y: 2, z: 4, core: 2. Of those that a mesh axis runs over, the one named last changes fastest.
Arguments:
- spectrum: float32 [256, 64, 64, 128], P('tmpl', 'grid'), may hold values from -12 to 12
Outputs:
- best_scores: float32 [4, 64, 64, 64], P(None, 'grid', 'tmpl')
- coherence: float32 [64, 64, 64], P('grid', 'tmpl')
The draws below stay inside these ranges and needn't reach their ends.
All inputs are finite; a program needn't handle non-finite values.
Results may differ from the reference program's by a relative error of at most 0.0001.
Values sent between devices are 32-bit elements; how exact they have to be, the bound alone decides.
A program may use at most 128 MiB of HBM per device.

```python
import math
import jax
import jax.numpy as jnp
from jax import lax

NG = 64
TEMPLATES = 256
TOP = 4


def log_uniform(key, shape, low, high):
    return jnp.exp(jax.random.uniform(key, shape, jnp.float32, math.log(low), math.log(high)))


def draw_spectrum(key, part):
    streams = jax.random.split(jax.random.fold_in(key, 11), 8)
    shape = (TEMPLATES, NG, NG, 2 * NG)
    base = jnp.clip(0.125 * jax.random.normal(streams[0], shape, jnp.float32), -0.75, 0.75)
    factor = log_uniform(streams[1], (TEMPLATES, NG, 1, 1), 0.5, 2.0)
    offset = jax.random.normal(streams[3], (TEMPLATES, NG), jnp.float32)
    values = base * factor
    values = values.at[:, :, :, 0].add(offset[:, :, None])
    return jnp.clip(values, -12.0, 12.0)


def setup_inputs(seed: int = 0) -> dict:
    streams_of = jax.random.split(jax.random.key(seed), 2)
    spectrum = draw_spectrum(jax.random.fold_in(streams_of[1], 71), 0)
    return dict(spectrum=spectrum)


FLOOR = -1e+30
SPREAD_FLOOR = 0.25

def phase_table(length):
    order = jnp.arange(length, dtype=jnp.int32)
    turns = order[:, None] * order[None, :] % length
    angle = turns.astype(jnp.float32) * (2.0 * math.pi / length)
    return jnp.concatenate([jnp.cos(angle), -jnp.sin(angle)], axis=0)

def merge_top(former, latter):
    result = []
    for rank_out in range(len(former)):
        winner = jnp.maximum(former[rank_out], latter[rank_out])
        for rank_in in range(rank_out):
            winner = jnp.maximum(winner, jnp.minimum(former[rank_in], latter[rank_out - rank_in - 1]))
        result.append(winner)
    return tuple(result)

def reference(spectrum):
    table = phase_table(NG)
    cell_count = float(NG * NG * NG)

    def advance(carry, coeffs):
        leaders, running = carry
        score = jnp.dot(coeffs.reshape(NG * NG, 2 * NG), table, precision=lax.Precision.HIGHEST, preferred_element_type=jnp.float32).reshape(NG, NG, NG)
        average = jnp.sum(score) / cell_count
        centred = score - average
        spread = jnp.sum(centred * centred) / cell_count
        normed = centred / jnp.sqrt(spread + SPREAD_FLOOR)
        filler = jnp.full((NG, NG, NG), FLOOR, jnp.float32)
        single = (normed,) + tuple((filler for rank_in in range(TOP - 1)))
        return ((merge_top(leaders, single), running + normed), None)
    start = tuple((jnp.full((NG, NG, NG), FLOOR, jnp.float32) for rank_in in range(TOP)))
    (leaders, running), unused = lax.scan(advance, (start, jnp.zeros((NG, NG, NG), jnp.float32)), spectrum)
    return (jnp.stack(leaders, axis=0), running / math.sqrt(TEMPLATES))
```

```python
import functools
import math

import jax
import jax.numpy as jnp
import numpy as np
from jax import lax
from jax.experimental import pallas as pl
from jax.experimental.pallas import tpu as pltpu
from jax.sharding import PartitionSpec as P

TOP = 4
KEPT = TOP + 1
SPREAD_FLOOR = 0.25
CHUNKS = 4
BATCH = 2
MESH = pl.DeviceIdType.MESH


def phase_tables(points):
    order = np.arange(points)
    angle = (order[:, None] * order[None, :] % points) * (2.0 * math.pi / points)
    table = np.concatenate([np.cos(angle), -np.sin(angle)], axis=0)
    table = np.kron(np.eye(2), table).astype(np.float32)
    lead = table.astype(jnp.bfloat16)
    rest = (table - lead.astype(np.float32)).astype(jnp.bfloat16)
    return np.concatenate([lead, lead, rest], axis=0)


def order_pair(former, latter):
    return jnp.maximum(former, latter), jnp.minimum(former, latter)


def order_four(values):
    a, b = order_pair(values[0], values[1])
    c, d = order_pair(values[2], values[3])
    a, c = order_pair(a, c)
    b, d = order_pair(b, d)
    b, c = order_pair(b, c)
    return [a, b, c, d]


def merge_four(former, latter):
    a, b, c, d = (jnp.maximum(former[i], latter[TOP - 1 - i]) for i in range(TOP))
    a, c = order_pair(a, c)
    b, d = order_pair(b, d)
    a, b = order_pair(a, b)
    c, d = order_pair(c, d)
    return [a, b, c, d]


def merge_groups(former, latter):
    return merge_four(former[:TOP], latter[:TOP]) + [former[TOP] + latter[TOP]]


def kernel(
    groups, slabs, parts,
    spectrum_ref, table_ref, best_ref, coherence_ref,
    held, table, score, stats, gathered, average, scale, leaders, sibling, merged, arrived,
    held_sem, table_sem, stats_send, stats_recv, pair_send, pair_recv, far_send, far_recv,
):
    local_tmpl, slab_rows, beta_rows, doubled = spectrum_ref.shape
    points = doubled // 2
    half = slab_rows // 2
    chips = groups // 2
    piece = beta_rows // groups
    per_chunk = half // CHUNKS
    cell_count = float(points * points * points)

    place = lax.axis_index("tmpl")
    slab = lax.axis_index("grid")
    chip, core = place // 2, place % 2

    def fetch(number):
        return pltpu.make_async_copy(
            spectrum_ref.at[pl.ds(number * BATCH, BATCH)],
            held.at[pl.ds(number * BATCH, BATCH)],
            held_sem.at[number],
        )

    bring_table = pltpu.make_async_copy(table_ref, table, table_sem)
    bring_table.start()
    for number in range(local_tmpl // BATCH):
        fetch(number).start()

    partner = (2 * chip + 1 - core, slab)
    far = [(2 * ((chip + step) % chips) + core, slab) for step in range(1, chips)]
    near = [(place, (slab + step) % slabs) for step in range(1, slabs)]
    barrier = pltpu.get_barrier_semaphore()
    for device in [partner] + far + near:
        pl.semaphore_signal(barrier, inc=1, device_id=device, device_id_type=MESH)

    bring_table.wait()

    def transform(number, carry):
        fetch(number).wait()
        base = number * BATCH
        rows = BATCH * half * beta_rows
        leads, rests = [], []
        for side in range(2):
            coeffs = held[pl.ds(base, BATCH), pl.ds(side * half, half)].reshape(rows, doubled)
            lead = coeffs.astype(jnp.bfloat16)
            leads.append(lead)
            rests.append((coeffs - lead.astype(jnp.float32)).astype(jnp.bfloat16))
        value = jnp.dot(
            jnp.concatenate(leads + rests + leads, axis=1),
            table[...],
            preferred_element_type=jnp.float32,
        )
        value = value.reshape(BATCH, half, beta_rows, doubled)
        score[pl.ds(base, BATCH)] = value
        for index in range(BATCH):
            one = value[index].reshape(half * beta_rows // 8, 8, doubled)
            plain = jnp.sum(jnp.sum(one, axis=0), axis=0, keepdims=True)
            square = jnp.sum(jnp.sum(one * one, axis=0), axis=0, keepdims=True)
            stats[0, pl.ds(base + index, 1)] = plain
            stats[1, pl.ds(base + index, 1)] = square
        return carry

    def share_stats(part):
        low, high = parts[part], parts[part + 1]
        return [
            pltpu.make_async_remote_copy(
                src_ref=stats.at[:, pl.ds(low, high - low)],
                dst_ref=gathered.at[step, :, pl.ds(low, high - low)],
                send_sem=stats_send.at[part, step],
                recv_sem=stats_recv.at[part, step],
                device_id=near[step],
                device_id_type=MESH,
            )
            for step in range(slabs - 1)
        ]

    def settle(part):
        low, size = parts[part], parts[part + 1] - parts[part]
        total = stats[:, pl.ds(low, size)]
        for step, copy in enumerate(share_stats(part)):
            copy.wait_recv()
            total = total + gathered[step, :, pl.ds(low, size)]
        total = jnp.sum(total, axis=-1, keepdims=True) / cell_count
        mean = total[0]
        spread = total[1] - mean * mean
        factor = 1.0 / jnp.sqrt(spread + SPREAD_FLOOR)
        average[pl.ds(low, size)] = jnp.broadcast_to(mean, (size, doubled))
        scale[pl.ds(low, size)] = jnp.broadcast_to(factor, (size, doubled))

    def leading(part, chunk):
        low, high = parts[part], parts[part + 1]

        def one_row(row, carry):
            line = chunk * per_chunk + row
            for pair in range(chips):
                window = pl.ds(pair * 2 * piece, 2 * piece)
                running = None
                for base in range(low, high, TOP):
                    values = []
                    for tmpl in range(base, base + TOP):
                        centred = score[tmpl, line, window] - average[pl.ds(tmpl, 1)]
                        values.append(centred * scale[pl.ds(tmpl, 1)])
                    summed = (values[0] + values[1]) + (values[2] + values[3])
                    fresh = order_four(values) + [summed]
                    running = fresh if running is None else merge_groups(running, fresh)
                for side in range(2):
                    rows = slice(side * piece, (side + 1) * piece)
                    mine = [value[rows] for value in running]
                    if part > 0:
                        former = [leaders[chunk, side, pair, rank, row] for rank in range(KEPT)]
                        mine = merge_groups(former, mine)
                    for rank in range(KEPT):
                        leaders[chunk, side, pair, rank, row] = mine[rank]
            return carry

        lax.fori_loop(0, per_chunk, one_row, 0)

    def exchange(chunk):
        return pltpu.make_async_remote_copy(
            src_ref=leaders.at[chunk, 1 - core],
            dst_ref=sibling.at[chunk],
            send_sem=pair_send.at[chunk],
            recv_sem=pair_recv.at[chunk],
            device_id=partner,
            device_id_type=MESH,
        )

    def scatter(chunk):
        return [
            pltpu.make_async_remote_copy(
                src_ref=merged.at[chunk, (chip + step) % chips],
                dst_ref=arrived.at[chunk, step - 1],
                send_sem=far_send.at[chunk, step - 1],
                recv_sem=far_recv.at[chunk, step - 1],
                device_id=far[step - 1],
                device_id_type=MESH,
            )
            for step in range(1, chips)
        ]

    def join_pair(chunk):
        exchange(chunk).wait_recv()
        for pair in range(chips):
            former = [leaders[chunk, core, pair, rank] for rank in range(KEPT)]
            latter = [sibling[chunk, pair, rank] for rank in range(KEPT)]
            for rank, value in enumerate(merge_groups(former, latter)):
                merged[chunk, pair, rank] = value
        for copy in scatter(chunk):
            copy.start()

    def finish(chunk):
        running = [merged[chunk, chip, rank] for rank in range(KEPT)]
        for step, copy in enumerate(scatter(chunk)):
            copy.wait_recv()
            running = merge_groups(
                running, [arrived[chunk, step, rank] for rank in range(KEPT)]
            )
        running[TOP] = running[TOP] / math.sqrt(groups * local_tmpl)
        for side in range(2):
            rows = pl.ds(side * half + chunk * per_chunk, per_chunk)
            lanes = slice(side * points, (side + 1) * points)
            for rank in range(TOP):
                best_ref[rank, rows] = running[rank][..., lanes]
            coherence_ref[rows] = running[TOP][..., lanes]

    count = len(parts) - 1
    for part in range(count):
        lax.fori_loop(parts[part] // BATCH, parts[part + 1] // BATCH, transform, 0)
        if part == 0:
            pl.semaphore_wait(barrier, 1 + len(far) + len(near))
        for copy in share_stats(part):
            copy.start()
    for part in range(count - 1):
        settle(part)
        for chunk in range(CHUNKS):
            leading(part, chunk)
    settle(count - 1)
    for chunk in range(CHUNKS):
        leading(count - 1, chunk)
        exchange(chunk).start()
        if chunk > 0:
            join_pair(chunk - 1)
    join_pair(CHUNKS - 1)
    for chunk in range(CHUNKS):
        finish(chunk)
    for part in range(count):
        for copy in share_stats(part):
            copy.wait_send()
    for chunk in range(CHUNKS):
        exchange(chunk).wait_send()
        for copy in scatter(chunk):
            copy.wait_send()


def body(groups, slabs, spectrum):
    local_tmpl, slab_rows, beta_rows, doubled = spectrum.shape
    points = doubled // 2
    half = slab_rows // 2
    chips = groups // 2
    piece = beta_rows // groups
    per_chunk = half // CHUNKS
    parts = (0, local_tmpl * 3 // 4, local_tmpl)
    count = len(parts) - 1
    block = (chips, KEPT, per_chunk, piece, doubled)
    f32 = jnp.float32
    dma = pltpu.SemaphoreType.DMA
    return pl.pallas_call(
        functools.partial(kernel, groups, slabs, parts),
        out_shape=(
            jax.ShapeDtypeStruct((TOP, slab_rows, piece, points), f32),
            jax.ShapeDtypeStruct((slab_rows, piece, points), f32),
        ),
        in_specs=[pl.BlockSpec(memory_space=pltpu.HBM)] * 2,
        out_specs=(
            pl.BlockSpec(memory_space=pltpu.VMEM),
            pl.BlockSpec(memory_space=pltpu.VMEM),
        ),
        scratch_shapes=[
            pltpu.VMEM((local_tmpl, slab_rows, beta_rows, doubled), f32),
            pltpu.VMEM((6 * doubled, doubled), jnp.bfloat16),
            pltpu.VMEM((local_tmpl, half, beta_rows, doubled), f32),
            pltpu.VMEM((2, local_tmpl, doubled), f32),
            pltpu.VMEM((slabs - 1, 2, local_tmpl, doubled), f32),
            pltpu.VMEM((local_tmpl, doubled), f32),
            pltpu.VMEM((local_tmpl, doubled), f32),
            pltpu.VMEM((CHUNKS, 2) + block, f32),
            pltpu.VMEM((CHUNKS,) + block, f32),
            pltpu.VMEM((CHUNKS,) + block, f32),
            pltpu.VMEM((CHUNKS, chips - 1) + block[1:], f32),
            dma((local_tmpl // BATCH,)),
            dma,
            dma((count, slabs - 1)),
            dma((count, slabs - 1)),
            dma((CHUNKS,)),
            dma((CHUNKS,)),
            dma((CHUNKS, chips - 1)),
            dma((CHUNKS, chips - 1)),
        ],
        compiler_params=pltpu.CompilerParams(
            collective_id=0, has_side_effects=True, vmem_limit_bytes=60 * 1024 * 1024
        ),
    )(spectrum, jnp.asarray(phase_tables(points)))


def solution(mesh):
    return jax.shard_map(
        functools.partial(body, mesh.shape["tmpl"], mesh.shape["grid"]),
        mesh=mesh,
        in_specs=(P("tmpl", "grid", None, None),),
        out_specs=(P(None, "grid", "tmpl", None), P("grid", "tmpl", None)),
        check_vma=False,
    )
```

```python
import functools
import math

import jax
import jax.numpy as jnp
import numpy as np
from jax import lax
from jax.experimental import pallas as pl
from jax.experimental.pallas import tpu as pltpu
from jax.sharding import PartitionSpec as P

TOP = 4
KEPT = TOP + 1
SPREAD_FLOOR = 0.25
CHUNKS = 4
BATCH = 8
AHEAD = 4
MB = 256
MESH = pl.DeviceIdType.MESH


def phase_tables(points):
    order = np.arange(points)
    angle = (order[:, None] * order[None, :] % points) * (2.0 * math.pi / points)
    table = np.concatenate([np.cos(angle), -np.sin(angle)], axis=0)
    table = np.kron(np.eye(2), table).astype(np.float32)
    lead = table.astype(jnp.bfloat16)
    rest = (table - lead.astype(np.float32)).astype(jnp.bfloat16)
    return np.concatenate([lead, rest], axis=1)


def order_pair(former, latter):
    return jnp.maximum(former, latter), jnp.minimum(former, latter)


def order_four(values):
    a, b = order_pair(values[0], values[1])
    c, d = order_pair(values[2], values[3])
    a, c = order_pair(a, c)
    b, d = order_pair(b, d)
    b, c = order_pair(b, c)
    return [a, b, c, d]


def merge_four(former, latter):
    a, b, c, d = (jnp.maximum(former[i], latter[TOP - 1 - i]) for i in range(TOP))
    a, c = order_pair(a, c)
    b, d = order_pair(b, d)
    a, b = order_pair(a, b)
    c, d = order_pair(c, d)
    return [a, b, c, d]


def merge_groups(former, latter):
    return merge_four(former[:TOP], latter[:TOP]) + [former[TOP] + latter[TOP]]


def kernel(
    groups, slabs, parts,
    spectrum_ref, table_ref, packed_ref,
    held, table, score, stats, gathered, average, scale, leaders, sibling, merged, arrived,
    held_sem, table_sem, stats_send, stats_recv, pair_send, pair_recv, far_send, far_recv,
):
    local_tmpl, slab_rows, beta_rows, doubled = spectrum_ref.shape
    points = doubled // 2
    half = slab_rows // 2
    chips = groups // 2
    piece = beta_rows // groups
    per_chunk = half // CHUNKS
    cell_count = float(points * points * points)

    place = lax.axis_index("tmpl")
    slab = lax.axis_index("grid")
    chip, core = place // 2, place % 2

    def fetch(number):
        return pltpu.make_async_copy(
            spectrum_ref.at[pl.ds(number * BATCH, BATCH)],
            held.at[pl.ds(number * BATCH, BATCH)],
            held_sem.at[number],
        )

    bring_table = pltpu.make_async_copy(table_ref, table, table_sem)
    bring_table.start()
    for number in range(min(AHEAD, local_tmpl // BATCH)):
        fetch(number).start()

    partner = (2 * chip + 1 - core, slab)
    far = [(2 * ((chip + step) % chips) + core, slab) for step in range(1, chips)]
    near = [(place, (slab + step) % slabs) for step in range(1, slabs)]
    barrier = pltpu.get_barrier_semaphore()
    for device in [partner] + far + near:
        pl.semaphore_signal(barrier, inc=1, device_id=device, device_id_type=MESH)

    bring_table.wait()

    def transform(number, carry):
        fetch(number).wait()

        @pl.when(number + AHEAD < local_tmpl // BATCH)
        def _():
            fetch(number + AHEAD).start()

        base = number * BATCH
        lines = MB // beta_rows
        for index in range(BATCH):
            plain = square = None
            for block in range(half // lines):
                leads, rests = [], []
                for side in range(2):
                    coeffs = held[base + index, pl.ds(side * half + block * lines, lines)].reshape(MB, doubled)
                    lead = coeffs.astype(jnp.bfloat16)
                    leads.append(lead)
                    rests.append((coeffs - lead.astype(jnp.float32)).astype(jnp.bfloat16))
                both = jnp.dot(jnp.concatenate(leads, axis=1), table[...], preferred_element_type=jnp.float32)
                value = both[:, :doubled] + both[:, doubled:] + jnp.dot(jnp.concatenate(rests, axis=1), table[:, :doubled], preferred_element_type=jnp.float32)
                score[base + index, pl.ds(block * lines, lines)] = value.reshape(lines, beta_rows, doubled)
                one = value.reshape(MB // 8, 8, doubled)
                p = jnp.sum(one, axis=0)
                q = jnp.sum(one * one, axis=0)
                plain = p if plain is None else plain + p
                square = q if square is None else square + q
            stats[0, pl.ds(base + index, 1)] = jnp.sum(plain, axis=0, keepdims=True)
            stats[1, pl.ds(base + index, 1)] = jnp.sum(square, axis=0, keepdims=True)
        return carry

    def share_stats(part):
        low, high = parts[part], parts[part + 1]
        return [
            pltpu.make_async_remote_copy(
                src_ref=stats.at[:, pl.ds(low, high - low)],
                dst_ref=gathered.at[step, :, pl.ds(low, high - low)],
                send_sem=stats_send.at[part, step],
                recv_sem=stats_recv.at[part, step],
                device_id=near[step],
                device_id_type=MESH,
            )
            for step in range(slabs - 1)
        ]

    def settle(part):
        low, size = parts[part], parts[part + 1] - parts[part]
        total = stats[:, pl.ds(low, size)]
        for step, copy in enumerate(share_stats(part)):
            copy.wait_recv()
            total = total + gathered[step, :, pl.ds(low, size)]
        total = jnp.sum(total, axis=-1, keepdims=True) / cell_count
        mean = total[0]
        spread = total[1] - mean * mean
        factor = 1.0 / jnp.sqrt(spread + SPREAD_FLOOR)
        average[pl.ds(low, size)] = jnp.broadcast_to(mean, (size, doubled))
        scale[pl.ds(low, size)] = jnp.broadcast_to(factor, (size, doubled))

    def leading(part, chunk):
        low, high = parts[part], parts[part + 1]

        def one_row(row, carry):
            line = chunk * per_chunk + row
            for pair in range(chips):
                window = pl.ds(pair * 2 * piece, 2 * piece)
                running = None
                for base in range(low, high, TOP):
                    values = []
                    for tmpl in range(base, base + TOP):
                        centred = score[tmpl, line, window] - average[pl.ds(tmpl, 1)]
                        values.append(centred * scale[pl.ds(tmpl, 1)])
                    summed = (values[0] + values[1]) + (values[2] + values[3])
                    fresh = order_four(values) + [summed]
                    running = fresh if running is None else merge_groups(running, fresh)
                for side in range(2):
                    rows = slice(side * piece, (side + 1) * piece)
                    mine = [value[rows] for value in running]
                    if part > 0:
                        former = [leaders[chunk, side, pair, rank, row] for rank in range(KEPT)]
                        mine = merge_groups(former, mine)
                    for rank in range(KEPT):
                        leaders[chunk, side, pair, rank, row] = mine[rank]
            return carry

        lax.fori_loop(0, per_chunk, one_row, 0)

    def exchange(chunk):
        return pltpu.make_async_remote_copy(
            src_ref=leaders.at[chunk, 1 - core],
            dst_ref=sibling.at[chunk],
            send_sem=pair_send.at[chunk],
            recv_sem=pair_recv.at[chunk],
            device_id=partner,
            device_id_type=MESH,
        )

    def scatter(chunk):
        return [
            pltpu.make_async_remote_copy(
                src_ref=merged.at[chunk, (chip + step) % chips],
                dst_ref=arrived.at[chunk, step - 1],
                send_sem=far_send.at[chunk, step - 1],
                recv_sem=far_recv.at[chunk, step - 1],
                device_id=far[step - 1],
                device_id_type=MESH,
            )
            for step in range(1, chips)
        ]

    def join_pair(chunk):
        exchange(chunk).wait_recv()
        for pair in range(chips):
            former = [leaders[chunk, core, pair, rank] for rank in range(KEPT)]
            latter = [sibling[chunk, pair, rank] for rank in range(KEPT)]
            for rank, value in enumerate(merge_groups(former, latter)):
                merged[chunk, pair, rank] = value
        for copy in scatter(chunk):
            copy.start()

    def finish(chunk):
        running = [merged[chunk, chip, rank] for rank in range(KEPT)]
        for step, copy in enumerate(scatter(chunk)):
            copy.wait_recv()
            running = merge_groups(
                running, [arrived[chunk, step, rank] for rank in range(KEPT)]
            )
        running[TOP] = running[TOP] / math.sqrt(groups * local_tmpl)
        for rank in range(KEPT):
            packed_ref[rank, pl.ds(chunk * per_chunk, per_chunk)] = running[rank]

    count = len(parts) - 1
    for part in range(count):
        lax.fori_loop(parts[part] // BATCH, parts[part + 1] // BATCH, transform, 0)
        if part == 0:
            pl.semaphore_wait(barrier, 1 + len(far) + len(near))
        for copy in share_stats(part):
            copy.start()
    for part in range(count - 1):
        settle(part)
        for chunk in range(CHUNKS):
            leading(part, chunk)
    settle(count - 1)
    for chunk in range(CHUNKS):
        leading(count - 1, chunk)
        exchange(chunk).start()
        if chunk > 0:
            join_pair(chunk - 1)
    join_pair(CHUNKS - 1)
    for chunk in range(CHUNKS):
        finish(chunk)
    for part in range(count):
        for copy in share_stats(part):
            copy.wait_send()
    for chunk in range(CHUNKS):
        exchange(chunk).wait_send()
        for copy in scatter(chunk):
            copy.wait_send()


def unpack(packed_ref, best_ref, coherence_ref):
    half, points = packed_ref.shape[1], best_ref.shape[-1]
    for side in range(2):
        rows = pl.ds(side * half, half)
        lanes = slice(side * points, (side + 1) * points)
        best_ref[:, rows] = packed_ref[:TOP, :, :, lanes]
        coherence_ref[rows] = packed_ref[TOP, :, :, lanes]


def body(groups, slabs, spectrum):
    local_tmpl, slab_rows, beta_rows, doubled = spectrum.shape
    points = doubled // 2
    half = slab_rows // 2
    chips = groups // 2
    piece = beta_rows // groups
    per_chunk = half // CHUNKS
    parts = (0, local_tmpl // 2, local_tmpl)
    count = len(parts) - 1
    block = (chips, KEPT, per_chunk, piece, doubled)
    f32 = jnp.float32
    dma = pltpu.SemaphoreType.DMA
    packed = pl.pallas_call(
        functools.partial(kernel, groups, slabs, parts),
        out_shape=jax.ShapeDtypeStruct((KEPT, half, piece, doubled), f32),
        in_specs=[pl.BlockSpec(memory_space=pltpu.HBM)] * 2,
        out_specs=pl.BlockSpec(memory_space=pltpu.VMEM),
        scratch_shapes=[
            pltpu.VMEM((local_tmpl, slab_rows, beta_rows, doubled), f32),
            pltpu.VMEM((2 * doubled, 2 * doubled), jnp.bfloat16),
            pltpu.VMEM((local_tmpl, half, beta_rows, doubled), f32),
            pltpu.VMEM((2, local_tmpl, doubled), f32),
            pltpu.VMEM((slabs - 1, 2, local_tmpl, doubled), f32),
            pltpu.VMEM((local_tmpl, doubled), f32),
            pltpu.VMEM((local_tmpl, doubled), f32),
            pltpu.VMEM((CHUNKS, 2) + block, f32),
            pltpu.VMEM((CHUNKS,) + block, f32),
            pltpu.VMEM((CHUNKS,) + block, f32),
            pltpu.VMEM((CHUNKS, chips - 1) + block[1:], f32),
            dma((local_tmpl // BATCH,)),
            dma,
            dma((count, slabs - 1)),
            dma((count, slabs - 1)),
            dma((CHUNKS,)),
            dma((CHUNKS,)),
            dma((CHUNKS, chips - 1)),
            dma((CHUNKS, chips - 1)),
        ],
        compiler_params=pltpu.CompilerParams(
            collective_id=0, has_side_effects=True, vmem_limit_bytes=60 * 1024 * 1024
        ),
    )(spectrum, jnp.asarray(phase_tables(points)))
    return pl.pallas_call(
        unpack,
        out_shape=(
            jax.ShapeDtypeStruct((TOP, slab_rows, piece, points), f32),
            jax.ShapeDtypeStruct((slab_rows, piece, points), f32),
        ),
    )(packed)


def solution(mesh):
    return jax.shard_map(
        functools.partial(body, mesh.shape["tmpl"], mesh.shape["grid"]),
        mesh=mesh,
        in_specs=(P("tmpl", "grid", None, None),),
        out_specs=(P(None, "grid", "tmpl", None), P("grid", "tmpl", None)),
        check_vma=False,
    )
```
